32 devices in a mesh: dp: 4 (over x, core), seq: 8 (over z, y).
Axes of the slice: x: 2, y: 2, z: 4, core: 2. Of those that a mesh axis runs over, the one named last changes fastest.
Arguments:
- block_input: bfloat16 [16384, 2560], P(('dp', 'seq')), may hold values from -6 to 6
- w_query: bfloat16 [2560, 2560], P('dp', 'seq'), may hold values from -4 to 4
- w_keyval: bfloat16 [2560, 512], P('dp', 'seq'), may hold values from -0.125 to 0.125
- w_out: bfloat16 [2560, 2560], P('dp', 'seq'), may hold values from -2 to 2
- gain_attn: bfloat16 [2560], P(('dp', 'seq')), may hold values from 0.5 to 1.5
- w_gate: bfloat16 [2560, 7680], P('dp', 'seq'), may hold values from -0.125 to 0.125
- w_up: bfloat16 [2560, 7680], P('dp', 'seq'), may hold values from -0.125 to 0.125
- w_down: bfloat16 [2560, 7680], P('dp', 'seq'), may hold values from -0.0625 to 0.0625
- gain_mlp: bfloat16 [2560], P(('dp', 'seq')), may hold values from 0.5 to 1.5
- cotangent: bfloat16 [16384, 2560], P(('dp', 'seq')), may hold values from -6 to 6
Outputs:
- output_rows: bfloat16 [16384, 2560], P(('dp', 'seq'))
- grad_input: float32 [16384, 2560], P(('dp', 'seq'))
- grad_w_query: float32 [2560, 2560], P('dp', 'seq')
- grad_w_keyval: float32 [2560, 512], P('dp', 'seq')
- grad_w_out: float32 [2560, 2560], P('dp', 'seq')
- grad_gain_attn: float32 [2560], P(('dp', 'seq'))
- grad_w_gate: float32 [2560, 7680], P('dp', 'seq')
- grad_w_up: float32 [2560, 7680], P('dp', 'seq')
- grad_w_down: float32 [2560, 7680], P('dp', 'seq')
- grad_gain_mlp: float32 [2560], P(('dp', 'seq'))
The draws below stay inside these ranges and needn't reach their ends.
All inputs are finite; a program needn't handle non-finite values.
Results may differ from the reference program's by a relative error of at most 0.019.
The reference program's roundings to bfloat16 on the way count: a program that leaves them out, or rounds other values in their place, can miss the bound.
Values may be sent and summed in bfloat16 or wider, within the bound.
A program may use at most 576 MiB of HBM per device.

```python
import math
import jax
import jax.numpy as jnp
from jax import lax

D = 2560
HEADS = 10
HD = 256
FF = 7680
WINDOW = 2048
LENGTH = 4096
TOKENS = 16384
N_DP = 4


def draw_w_query(key, part):
    base_key = jax.random.fold_in(key, 11)
    factor_key = jax.random.fold_in(key, 12)
    base = jax.random.normal(base_key, (D, HEADS * HD), jnp.float32) * D ** (-0.5)
    factor = jnp.exp(jax.random.uniform(factor_key, (HEADS,), jnp.float32, jnp.log(0.5), jnp.log(2.0)))
    return jnp.clip(base * jnp.repeat(factor, HD)[None, :], -4.0, 4.0).astype(jnp.bfloat16)


def steps_of(stream_key, shape, split, smallest, high):
    level, own = 1.0, jax.random.fold_in(stream_key, 6)
    for dim, blocks in split:
        heights = jnp.exp(jax.random.uniform(jax.random.fold_in(own, dim), (blocks,), jnp.float32, smallest / len(split), high / len(split)))
        level = level * jnp.repeat(heights, shape[dim] // blocks).reshape([-1 if axis == dim else 1 for axis in range(len(shape))])
    return level


def normal_values(stream_key, extent, spread, most, cuts=(), kind=jnp.bfloat16):
    factor_of = steps_of(stream_key, extent, cuts, -0.22, 0.18) if cuts else 1.0
    array = jax.random.normal(stream_key, extent, jnp.float32) * spread * factor_of
    return jnp.minimum(jnp.maximum(array, -most), most).astype(kind)


def setup_inputs(seed: int = 0) -> dict:
    splits = jax.random.split(jax.random.key(seed), 11)
    block_input = normal_values(splits[0], (TOKENS, D), 1.0, 6.0, ((0, 32),))
    w_query = draw_w_query(jax.random.fold_in(splits[10], 71), 0)
    w_keyval = normal_values(splits[2], (D, 2 * HD), D ** -0.5, 0.125, ((0, 4), (1, 8)))
    w_out = normal_values(splits[3], (D, HEADS * HD), (max(HEADS * HD // 256, 1)) ** -0.5, 2.0, ((0, 4), (1, 8)))
    gain_attn = jnp.clip(1.0 + 0.1 * jax.random.normal(splits[4], (D,), jnp.float32), 0.5, 1.5).astype(jnp.bfloat16)
    w_gate = normal_values(splits[5], (D, FF), D ** -0.5, 0.125, ((0, 4), (1, 8)))
    w_up = normal_values(splits[6], (D, FF), D ** -0.5, 0.125, ((0, 4), (1, 8)))
    w_down = normal_values(splits[7], (D, FF), FF ** -0.5, 0.0625, ((0, 4), (1, 8)))
    gain_mlp = jnp.clip(1.0 + 0.1 * jax.random.normal(splits[8], (D,), jnp.float32), 0.5, 1.5).astype(jnp.bfloat16)
    cotangent = normal_values(splits[9], (TOKENS, D), 1.0, 6.0, ((0, 32),))
    return {"block_input": block_input, "w_query": w_query, "w_keyval": w_keyval, "w_out": w_out, "gain_attn": gain_attn, "w_gate": w_gate, "w_up": w_up, "w_down": w_down, "gain_mlp": gain_mlp, "cotangent": cotangent}


@jax.custom_vjp
def low(v):
    return lax.optimization_barrier(v.astype(jnp.bfloat16)).astype(jnp.float32)

@jax.custom_vjp
def low_back(v):
    return v

def low_keep(v):
    return (low(v), None)

def low_pass(kept, grad):
    return (grad,)

def back_keep(v):
    return (v, None)

def back_low(kept, grad):
    return (low(grad),)
low.defvjp(low_keep, low_pass)
low_back.defvjp(back_keep, back_low)

def norm_rows(values, gain):
    return values * lax.rsqrt(lax.optimization_barrier(jnp.mean(values * values, axis=-1, keepdims=True)) + 1e-06) * gain

def rotate(values, positions):
    rope_width = values.shape[-1] // 2
    half_width = rope_width // 2
    frequency = 10000.0 ** (-jnp.arange(half_width, dtype=jnp.float32) / half_width)
    angles = positions.astype(jnp.float32)[:, None] * frequency[None, :]
    cosine = jnp.cos(angles)
    sine_part = jnp.sin(angles)
    first_half = values[..., :half_width]
    second_half = values[..., half_width:rope_width]
    unturned = values[..., rope_width:]
    return jnp.concatenate([first_half * cosine - second_half * sine_part, second_half * cosine + first_half * sine_part, unturned], axis=-1)

def gelu_tanh(v):
    return jax.nn.gelu(v, approximate=True)

def one_sequence(tokens, w_query, w_keyval, w_out, gain_attn, w_gate, w_up, w_down, gain_mlp):
    highest = lax.Precision.HIGHEST
    length = tokens.shape[0]
    positions = jnp.arange(length, dtype=jnp.int32)
    normed_one = low(norm_rows(tokens, gain_attn))
    query_raw = low_back(jnp.dot(normed_one, w_query, precision=highest))
    keyval_raw = low_back(jnp.dot(normed_one, w_keyval, precision=highest))
    query_heads = query_raw.reshape(length, HEADS, HD).transpose(1, 0, 2)
    queries = low(rotate(query_heads, positions))
    key_rows = low(rotate(keyval_raw[:, :HD], positions))
    value_rows = low(keyval_raw[:, HD:])
    block_rows = math.gcd(512, length)
    score_scale = HD ** (-0.5)

    def attend(block_index):
        first_row = block_index * block_rows
        query_block = lax.dynamic_slice_in_dim(queries, first_row, block_rows, 1)
        scores = jnp.einsum('hqd,kd->hqk', query_block, key_rows, precision=highest) * score_scale
        scores = low_back(scores)
        query_pos = first_row + jnp.arange(block_rows, dtype=jnp.int32)
        distance = query_pos[:, None] - positions[None, :]
        allowed = (distance >= 0) & (distance < WINDOW)
        scores = jnp.where(allowed[None], scores, -1e+30)
        row_max = lax.optimization_barrier(jnp.max(scores, axis=-1, keepdims=True))
        exponent = jnp.exp(scores - row_max)
        probs = exponent / lax.optimization_barrier(jnp.sum(exponent, axis=-1, keepdims=True))
        return jnp.einsum('hqk,kd->hqd', low(probs), value_rows, precision=highest)
    mixed_heads = lax.map(jax.checkpoint(attend), jnp.arange(length // block_rows, dtype=jnp.int32))
    mixed_heads = mixed_heads.transpose(0, 2, 1, 3).reshape(length, HEADS * HD)
    mixed_low = low(low_back(mixed_heads))
    resid = tokens + low_back(jnp.dot(mixed_low, w_out.T, precision=highest))
    normed_two = low(norm_rows(resid, gain_mlp))
    gate_pre = low_back(jnp.dot(normed_two, w_gate, precision=highest))
    upward = low_back(jnp.dot(normed_two, w_up, precision=highest))
    hidden = low(gelu_tanh(gate_pre) * upward)
    return resid + low_back(jnp.dot(hidden, w_down.T, precision=highest))

def reference(block_input, w_query, w_keyval, w_out, gain_attn, w_gate, w_up, w_down, gain_mlp, cotangent):
    weights = tuple((w.astype(jnp.float32) for w in (w_query, w_keyval, w_out, gain_attn, w_gate, w_up, w_down, gain_mlp)))
    inputs = block_input.astype(jnp.float32).reshape(N_DP, LENGTH, D)

    def forward(tokens, *params):

        def per_sequence(single):
            return one_sequence(single, *params)
        return lax.map(jax.checkpoint(per_sequence), tokens)
    result, pullback = jax.vjp(forward, inputs, *weights)
    gradients = pullback(cotangent.astype(jnp.float32).reshape(result.shape))
    output_rows = result.reshape(TOKENS, D).astype(jnp.bfloat16)
    return (output_rows, gradients[0].reshape(TOKENS, D), gradients[1], gradients[2], gradients[3], gradients[4], gradients[5], gradients[6], gradients[7], gradients[8])
```

```python
import jax
import jax.numpy as jnp
from jax import lax
from jax.sharding import Mesh
from jax.sharding import PartitionSpec as P

HEADS = 10
HD = 256
WINDOW = 2048
EPS = 1e-06

ALL = ("x", "c", "z", "y")
SWAP = [(0, 1), (1, 0)]
BF = jnp.bfloat16
F32 = jnp.float32


def norm_rows(values, gain):
    return values * lax.rsqrt(jnp.mean(values * values, axis=-1, keepdims=True) + EPS) * gain


def rotate(values, positions):
    rope_width = values.shape[-1] // 2
    half_width = rope_width // 2
    frequency = 10000.0 ** (-jnp.arange(half_width, dtype=F32) / half_width)
    angles = positions.astype(F32)[:, None] * frequency[None, :]
    cosine = jnp.cos(angles)
    sine_part = jnp.sin(angles)
    first_half = values[..., :half_width]
    second_half = values[..., half_width:rope_width]
    unturned = values[..., rope_width:]
    return jnp.concatenate(
        [
            first_half * cosine - second_half * sine_part,
            second_half * cosine + first_half * sine_part,
            unturned,
        ],
        axis=-1,
    )


def gelu_tanh(v):
    return jax.nn.gelu(v, approximate=True)


def dot(left, right, dims):
    return lax.dot_general(left, right, (dims, ((), ())), preferred_element_type=F32)


def rows_rows(left, right):
    return dot(left, right, ((0,), (0,)))


def last_last(left, right):
    return dot(left, right, ((1,), (1,)))


def swap(v, axis):
    return lax.ppermute(v, axis, SWAP)


def hop(v, by):
    length = lax.axis_size("z")
    return lax.ppermute(v, "z", [(i, i + by) for i in range(length) if 0 <= i + by < length])


def flip_if(odd, v, axis):
    return jnp.where(odd, jnp.flip(v, axis), v)


def gather_plane(v):
    half = v.shape[0] // 2
    over_x = swap(v, "x")
    over_y = swap(v, "y")
    corner = (swap(over_x[:half], "y"), swap(over_y[half:], "x"))
    corner = jnp.concatenate(corner, axis=0)
    blocks = {(0, 0): v, (1, 0): over_x, (0, 1): over_y, (1, 1): corner}
    return {k: (b, swap(b, "c")) for k, b in blocks.items()}


def scatter_plane(parts):
    def paired(k):
        return parts[k][0] + swap(parts[k][1], "c")

    corner, side_x, side_y, own = (paired(k) for k in ((1, 1), (1, 0), (0, 1), (0, 0)))
    half = own.shape[0] // 2
    a_own = own[:half] + swap(side_x[:half], "x")
    a_far = side_y[:half] + swap(corner[:half], "x")
    b_own = own[half:] + swap(side_y[half:], "y")
    b_far = side_x[half:] + swap(corner[half:], "y")
    return jnp.concatenate(
        [
            a_own.astype(F32) + swap(a_far, "y").astype(F32),
            b_own.astype(F32) + swap(b_far, "x").astype(F32),
        ],
        axis=0,
    )


def local(
    block_input, w_query, w_keyval, w_out, gain_attn, w_gate, w_up, w_down, gain_mlp, cotangent
):
    rows, width = block_input.shape
    z_size = lax.axis_size("z")
    ax, ac, az, ay = (lax.axis_index(n) for n in ALL)
    seq_place = 2 * az + ay
    odd_x, odd_c, odd_y = ax == 1, ac == 1, ay == 1
    depth = min((WINDOW + rows - 2) // rows, 2 * z_size - 1)
    pairs_back = (depth + 1) // 2
    score_scale = HD ** (-0.5)
    token = jnp.arange(rows, dtype=jnp.int32)
    positions = seq_place * rows + token
    dq, q_cols = w_query.shape
    kv_cols = w_keyval.shape[1]
    ff_cols = w_gate.shape[1]

    def rel_d(v):
        t = v.reshape(v.shape[0], 2, 2, dq)
        t = flip_if(odd_x, flip_if(odd_c, t, 2), 1)
        return t.reshape(v.shape)

    def to_rel_cols(v):
        n = v.shape[1] // (2 * z_size)
        t = v.reshape(v.shape[0], z_size, 2, n).transpose(0, 2, 1, 3)
        return flip_if(odd_y, t, 1).reshape(v.shape)

    def from_rel_cols(v):
        n = v.shape[1] // (2 * z_size)
        t = flip_if(odd_y, v.reshape(v.shape[0], 2, z_size, n), 1)
        return t.transpose(0, 2, 1, 3).reshape(v.shape)

    gains = lax.all_gather(jnp.stack([gain_attn, gain_mlp]), ALL, axis=1, tiled=True).astype(F32)
    gain_one, gain_two = gains[0], gains[1]

    def attn_weight(wt):
        n = wt.shape[0]
        stacked = lax.all_gather(wt, "z", axis=0, tiled=True)
        got = gather_plane(stacked)
        return {k: [p.reshape(z_size, n, dq) for p in v] for k, v in got.items()}

    def join(got, lo, hi):
        return jnp.concatenate(
            [
                jnp.concatenate(
                    [
                        got[(dx, dy)][dc][:, lo:hi].reshape(z_size * (hi - lo), dq)
                        for dx in (0, 1)
                        for dc in (0, 1)
                    ],
                    axis=1,
                )
                for dy in (0, 1)
            ],
            axis=0,
        )

    qkv_got = attn_weight(jnp.concatenate([w_query.T, w_keyval.T], axis=0))
    query_t = join(qkv_got, 0, q_cols)
    keyval_t = join(qkv_got, q_cols, q_cols + kv_cols)
    out_got = attn_weight(w_out.T)
    out_t = join(out_got, 0, q_cols)

    def split_hidden(w):
        n = ff_cols // 4
        t = w.T.reshape(2, 2, n, dq)
        t = flip_if(odd_x, flip_if(odd_c, t, 1), 0)
        kept, other = t[0], swap(t[1], "x")
        pieces = [kept[0], swap(kept[1], "c"), other[0], swap(other[1], "c")]
        piece = jnp.concatenate(pieces, axis=1)
        return rel_d(piece)

    def ff_weight(w):
        return lax.all_gather(split_hidden(w), "z", axis=0, tiled=True)

    gate_t, up_t, down_t = ff_weight(w_gate), ff_weight(w_up), ff_weight(w_down)

    inputs = block_input.astype(F32)
    normed_one_f, norm_one_pull = jax.vjp(norm_rows, inputs, gain_one)
    normed_one = rel_d(normed_one_f.astype(BF))
    keyval_raw = from_rel_cols(last_last(normed_one, keyval_t))
    query_raw = from_rel_cols(last_last(normed_one, query_t))

    def turn_rows(v):
        return rotate(v, positions)

    query_rot, query_pull = jax.vjp(
        turn_rows, query_raw.reshape(rows, HEADS, HD).transpose(1, 0, 2)
    )
    key_rot, key_pull = jax.vjp(turn_rows, keyval_raw[:, :HD])
    queries = query_rot.astype(BF).reshape(HEADS * rows, HD)
    keyval_own = jnp.concatenate([key_rot, keyval_raw[:, HD:]], axis=1).astype(BF)

    column = [keyval_own]
    for _ in range(pairs_back):
        column.append(hop(column[-1], 1))
    beside = [swap(c, "y") for c in column]

    def even_odd(j):
        return (
            jnp.where(odd_y, beside[j], column[j]),
            jnp.where(odd_y, column[j], beside[j]),
        )

    last_even, last_odd = even_odd(pairs_back)
    pieces = [keyval_own, jnp.where(odd_y, beside[0], last_even)]
    places = [seq_place, jnp.where(odd_y, seq_place - 1, 2 * (az - pairs_back))]
    for j in range(1, pairs_back):
        even, odd = even_odd(j)
        pieces += [odd, even]
        places += [2 * (az - j) + 1, 2 * (az - j)]
    pieces.append(last_odd)
    places.append(2 * (az - pairs_back) + 1)
    keyval_all = jnp.concatenate(pieces, axis=0)
    key_rows = keyval_all[:, :HD]
    value_rows = keyval_all[:, HD:]
    key_pos = (jnp.stack(places)[:, None] * rows + token[None, :]).reshape(-1)
    query_pos = jnp.tile(positions, HEADS)
    distance = query_pos[:, None] - key_pos[None, :]
    allowed = (distance >= 0) & (distance < WINDOW) & (key_pos[None, :] >= 0)

    def score_block():
        return jnp.where(allowed, last_last(queries, key_rows) * score_scale, -1e30)

    scores = score_block()
    row_max = jnp.max(scores, axis=1, keepdims=True)
    exponent = jnp.exp(scores - row_max)
    row_total = jnp.sum(exponent, axis=1, keepdims=True)
    probs = exponent / row_total
    log_total = row_max + jnp.log(row_total)
    mixed_heads = jnp.dot(probs.astype(BF), value_rows, preferred_element_type=F32)
    mixed_low = (
        mixed_heads.reshape(HEADS, rows, HD)
        .transpose(1, 0, 2)
        .reshape(rows, HEADS * HD)
        .astype(BF)
    )
    mixed_rel = to_rel_cols(mixed_low)
    resid = inputs + rel_d(dot(mixed_rel, out_t, ((1,), (0,))))
    normed_two_f, norm_two_pull = jax.vjp(norm_rows, resid, gain_two)
    normed_two = normed_two_f.astype(BF)

    cot_got = gather_plane(cotangent)
    norm_got = gather_plane(normed_two)
    order = ((0, 0), (1, 0), (0, 1), (1, 1))
    kept = {}
    for k in order:
        cot_g = jnp.concatenate(cot_got[k], axis=0)
        norm_g = jnp.concatenate(norm_got[k], axis=0)
        grad_hidden = last_last_t(cot_g, down_t)
        gate_pre = last_last(norm_g, gate_t)
        upward = last_last(norm_g, up_t)
        gelu_value, gelu_pull = jax.vjp(gelu_tanh, gate_pre)
        hidden = (gelu_value * upward).astype(BF)
        grad_gate = gelu_pull(grad_hidden * upward)[0].astype(BF)
        grad_upward = (grad_hidden * gelu_value).astype(BF)
        kept[k] = (cot_g, norm_g, hidden, grad_gate, grad_upward)

    back = {}
    for k in order[::-1]:
        _, _, _, grad_gate, grad_upward = kept[k]
        part = dot(grad_gate, gate_t, ((1,), (0,))) + dot(grad_upward, up_t, ((1,), (0,)))
        part = part.astype(BF)
        back[k] = (part[:rows], part[rows:])
    grad_normed_two = scatter_plane(back)
    ahead = {}
    for k in order[::-1]:
        part = dot(kept[k][2], down_t, ((1,), (0,))).astype(BF)
        ahead[k] = (part[:rows], part[rows:])
    output_rows = (resid + scatter_plane(ahead)).astype(BF)

    cot_all, norm_all, hidden_all, gate_all, upward_all = (
        jnp.concatenate([kept[k][i] for k in order], axis=0) for i in range(5)
    )

    def ff_grad(left, right):
        share = rows_rows(left, right).astype(BF)
        piece = rel_d(lax.psum_scatter(share, "z", scatter_dimension=0, tiled=True))
        n = piece.shape[0]
        t = piece.reshape(n, 2, 2, dq)
        mine = jnp.concatenate([t[:, 0, 0], swap(t[:, 0, 1], "c")], axis=0)
        far = jnp.concatenate([t[:, 1, 0], swap(t[:, 1, 1], "c")], axis=0)
        t = jnp.concatenate([mine, swap(far, "x")], axis=0).reshape(2, 2, n, dq)
        t = flip_if(odd_x, flip_if(odd_c, t, 1), 0)
        return t.reshape(4 * n, dq).T.astype(F32)

    grad_w_gate = ff_grad(gate_all, norm_all)
    grad_w_up = ff_grad(upward_all, norm_all)
    grad_w_down = ff_grad(hidden_all, cot_all)

    grad_resid_part, grad_gain_two = norm_two_pull(grad_normed_two)
    grad_resid = cotangent.astype(F32) + grad_resid_part
    attn_low = rel_d(grad_resid.astype(BF))

    def attn_grad(cols, d_rows):
        per = cols.shape[1] // 2
        parts = {}
        for dx in (0, 1):
            both = [
                rows_rows(cols, d_rows[:, (2 * dx + dc) * dq : (2 * dx + dc + 1) * dq]).astype(BF)
                for dc in (0, 1)
            ]
            for dy in (0, 1):
                parts[(dx, dy)] = tuple(b[dy * per : (dy + 1) * per] for b in both)
        summed = scatter_plane(parts).astype(BF)
        return lax.psum_scatter(summed, "z", scatter_dimension=0, tiled=True).astype(F32)

    grad_w_out = attn_grad(mixed_rel, attn_low).T
    grad_mixed = from_rel_cols(last_last(attn_low, out_t).astype(BF))
    grad_heads = grad_mixed.reshape(rows, HEADS, HD).transpose(1, 0, 2).reshape(HEADS * rows, HD)
    probs_again = jnp.exp(score_block() - log_total)
    grad_probs = last_last(grad_heads, value_rows)
    grad_scores = (
        probs_again * (grad_probs - jnp.sum(probs_again * grad_probs, axis=1, keepdims=True))
    ).astype(BF)
    grad_keys_all = rows_rows(grad_scores, queries) * score_scale
    grad_values_all = rows_rows(probs_again.astype(BF), grad_heads)
    grad_queries = jnp.dot(grad_scores, key_rows, preferred_element_type=F32) * score_scale
    grad_pieces = jnp.concatenate([grad_keys_all, grad_values_all], axis=1).reshape(
        -1, rows, 2 * HD
    )

    second = grad_pieces[1]
    zero = jnp.zeros_like(second)
    for_column = [grad_pieces[0]]
    for_beside = [jnp.where(odd_y, second, zero)]
    for j in range(1, pairs_back):
        odd, even = grad_pieces[2 * j], grad_pieces[2 * j + 1]
        for_column.append(jnp.where(odd_y, odd, even))
        for_beside.append(jnp.where(odd_y, even, odd))
    last = grad_pieces[-1]
    for_column.append(jnp.where(odd_y, last, second))
    for_beside.append(jnp.where(odd_y, zero, last))
    returned = zero
    for j in range(pairs_back, -1, -1):
        here = for_column[j] + swap(for_beside[j].astype(BF), "y").astype(F32)
        if j < pairs_back:
            here = here + hop(returned.astype(BF), -1).astype(F32)
        returned = here
    grad_keyval = returned
    grad_keys_raw = key_pull(grad_keyval[:, :HD])[0]
    grad_keyval_raw = to_rel_cols(
        jnp.concatenate([grad_keys_raw, grad_keyval[:, HD:]], axis=1).astype(BF)
    )
    grad_query_raw = to_rel_cols(
        query_pull(grad_queries.reshape(HEADS, rows, HD))[0]
        .transpose(1, 0, 2)
        .reshape(rows, HEADS * HD)
        .astype(BF)
    )
    grad_w_query = attn_grad(grad_query_raw, normed_one).T
    grad_w_keyval = attn_grad(grad_keyval_raw, normed_one).T
    grad_normed_one = rel_d(
        dot(grad_query_raw, query_t, ((1,), (0,))) + dot(grad_keyval_raw, keyval_t, ((1,), (0,)))
    )
    grad_in_part, grad_gain_one = norm_one_pull(grad_normed_one)
    grad_input = grad_resid + grad_in_part
    gain_shares = (
        lax.psum_scatter(grad_gain_one, ALL, scatter_dimension=0, tiled=True),
        lax.psum_scatter(grad_gain_two, ALL, scatter_dimension=0, tiled=True),
    )
    return (
        output_rows,
        grad_input,
        grad_w_query,
        grad_w_keyval,
        grad_w_out,
        gain_shares[0],
        grad_w_gate,
        grad_w_up,
        grad_w_down,
        gain_shares[1],
    )


def last_last_t(left, right_t):
    return dot(left, right_t, ((1,), (1,)))


def solution(mesh):
    n_dp, n_seq = mesh.shape["dp"], mesh.shape["seq"]
    fine = Mesh(mesh.devices.reshape(n_dp // 2, 2, n_seq // 2, 2), ALL)
    tokens = P(ALL, None)
    weight = P(("x", "c"), ("z", "y"))
    gain = P(ALL)
    return jax.shard_map(
        local,
        mesh=fine,
        in_specs=(
            tokens, weight, weight, weight, gain, weight, weight, weight, gain, tokens,
        ),
        out_specs=(
            tokens, tokens, weight, weight, weight, gain, weight, weight, weight, gain,
        ),
        check_vma=False,
    )
```

```python
import jax
import jax.numpy as jnp
from jax import lax
from jax.sharding import Mesh
from jax.sharding import PartitionSpec as P

HEADS = 10
HD = 256
WINDOW = 2048
EPS = 1e-06

ALL = ("x", "c", "z", "y")
SWAP = [(0, 1), (1, 0)]
BF = jnp.bfloat16
F32 = jnp.float32


def norm_rows(values, gain):
    return values * lax.rsqrt(jnp.mean(values * values, axis=-1, keepdims=True) + EPS) * gain


def rotate(values, positions):
    rope_width = values.shape[-1] // 2
    half_width = rope_width // 2
    frequency = 10000.0 ** (-jnp.arange(half_width, dtype=F32) / half_width)
    angles = positions.astype(F32)[:, None] * frequency[None, :]
    cosine = jnp.cos(angles)
    sine_part = jnp.sin(angles)
    first_half = values[..., :half_width]
    second_half = values[..., half_width:rope_width]
    unturned = values[..., rope_width:]
    return jnp.concatenate(
        [
            first_half * cosine - second_half * sine_part,
            second_half * cosine + first_half * sine_part,
            unturned,
        ],
        axis=-1,
    )


def gelu_tanh(v):
    return jax.nn.gelu(v, approximate=True)


def dot(left, right, dims):
    return lax.dot_general(left, right, (dims, ((), ())), preferred_element_type=F32)


def rows_rows(left, right):
    return dot(left, right, ((0,), (0,)))


def last_last(left, right):
    return dot(left, right, ((1,), (1,)))


def swap(v, axis):
    return lax.ppermute(v, axis, SWAP)


def hop(v, by):
    length = lax.axis_size("z")
    return lax.ppermute(v, "z", [(i, i + by) for i in range(length) if 0 <= i + by < length])


def pick(odd, first, second):
    return jnp.where(odd, second, first), jnp.where(odd, first, second)


def after(values, *earlier):
    return lax.optimization_barrier((values, earlier))[0]


def gather_plane(v):
    half = v.shape[0] // 2
    over_x = swap(v, "x")
    over_y = swap(v, "y")
    corner = (swap(over_x[:half], "y"), swap(over_y[half:], "x"))
    corner = jnp.concatenate(corner, axis=0)
    got = {}
    for (dx, dy), b in (((0, 0), v), ((1, 0), over_x), ((0, 1), over_y), ((1, 1), corner)):
        got[dx, dy, 0] = b
        got[dx, dy, 1] = swap(b, "c")
    return got


def scatter_plane(parts):
    def paired(k):
        return parts[k][0] + swap(parts[k][1], "c")

    corner, side_x, side_y, own = (paired(k) for k in ((1, 1), (1, 0), (0, 1), (0, 0)))
    half = own.shape[0] // 2
    a_own = own[:half] + swap(side_x[:half], "x")
    a_far = side_y[:half] + swap(corner[:half], "x")
    b_own = own[half:] + swap(side_y[half:], "y")
    b_far = side_x[half:] + swap(corner[half:], "y")
    return jnp.concatenate(
        [
            a_own.astype(F32) + swap(a_far, "y").astype(F32),
            b_own.astype(F32) + swap(b_far, "x").astype(F32),
        ],
        axis=0,
    )


def local(
    block_input, w_query, w_keyval, w_out, gain_attn, w_gate, w_up, w_down, gain_mlp, cotangent
):
    rows, width = block_input.shape
    z_size = lax.axis_size("z")
    ax, ac, az, ay = (lax.axis_index(n) for n in ALL)
    seq_place = 2 * az + ay
    odd_x, odd_c, odd_y = ax == 1, ac == 1, ay == 1
    depth = min((WINDOW + rows - 2) // rows, 2 * z_size - 1)
    pairs_back = (depth + 1) // 2
    score_scale = HD ** (-0.5)
    token = jnp.arange(rows, dtype=jnp.int32)
    positions = seq_place * rows + token
    dq, q_cols = w_query.shape
    kv_cols = w_keyval.shape[1]
    ff_cols = w_gate.shape[1]

    n_gain = gain_attn.shape[0]
    qkv_cols = q_cols + kv_cols

    def rel_blocks(v):
        b = [v[:, i * dq : (i + 1) * dq] for i in range(4)]
        top, low = pick(odd_c, b[0], b[1]), pick(odd_c, b[2], b[3])
        (b00, b10), (b01, b11) = pick(odd_x, top[0], low[0]), pick(odd_x, top[1], low[1])
        return {(0, 0): b00, (0, 1): b01, (1, 0): b10, (1, 1): b11}

    def abs_width(b):
        top = pick(odd_c, b[0, 0], b[0, 1])
        low = pick(odd_c, b[1, 0], b[1, 1])
        (a0, a2), (a1, a3) = pick(odd_x, top[0], low[0]), pick(odd_x, top[1], low[1])
        return jnp.concatenate([a0, a1, a2, a3], axis=1)

    def rel_cols(v):
        t = v.reshape(rows, z_size, 2, -1)
        return pick(odd_y, t[:, :, 0], t[:, :, 1])

    def abs_cols(v):
        return jnp.stack(pick(odd_y, v[0], v[1]), axis=2).reshape(rows, -1)

    extra = 16
    gain_row = jnp.zeros((extra, dq), BF)
    gain_row = gain_row.at[0, :n_gain].set(gain_attn).at[1, :n_gain].set(gain_mlp)
    qkv_own = jnp.concatenate([w_query.T, w_keyval.T, gain_row], axis=0)
    qkv_z = lax.all_gather(qkv_own, "z", axis=0, tiled=True)
    qkv_w = gather_plane(qkv_z)
    out_z = lax.all_gather(after(w_out, qkv_z).T, "z", axis=0, tiled=True)
    out_w = gather_plane(after(out_z, *(qkv_w[1, 1, c] for c in (0, 1))))
    row_size = qkv_cols + extra

    def gain_of(r):
        by = {
            k: v.reshape(z_size, row_size, dq)[:, qkv_cols + r, :n_gain] for k, v in qkv_w.items()
        }
        wide = {}
        for dx in (0, 1):
            for dc in (0, 1):
                pair = pick(odd_y, by[dx, 0, dc], by[dx, 1, dc])
                wide[dx, dc] = jnp.stack(pair, axis=1).reshape(1, dq)
        return abs_width(wide).reshape(-1).astype(F32)

    gain_one, gain_two = gain_of(0), gain_of(1)

    n_hidden = ff_cols // 4

    def ff_weight(w):
        t = lax.all_to_all(
            w.T.reshape(4, n_hidden, dq), ("x", "c"), split_axis=0, concat_axis=0, tiled=True
        )
        piece = t.transpose(1, 0, 2).reshape(n_hidden, width)
        return lax.all_gather(piece, "z", axis=0, tiled=True)

    down_t, gate_t, up_t = ff_weight(w_down), ff_weight(w_gate), ff_weight(w_up)

    def times(blocks, weights):
        out = []
        for dy in (0, 1):
            total = 0.0
            for (dx, dc), b in blocks.items():
                total = total + last_last(b, weights[dx, dy, dc])
            out.append(total)
        return out

    def times_t(cols, weights):
        return {
            (dx, dc): sum(dot(cols[dy], weights[dx, dy, dc], ((1,), (0,))) for dy in (0, 1))
            for dx in (0, 1)
            for dc in (0, 1)
        }

    inputs = block_input.astype(F32)
    normed_one_f, norm_one_pull = jax.vjp(norm_rows, inputs, gain_one)
    normed_one = rel_blocks(normed_one_f.astype(BF))
    qkv_rel = [v.reshape(rows, z_size, row_size) for v in times(normed_one, qkv_w)]
    query_raw = abs_cols([v[:, :, :q_cols] for v in qkv_rel])
    keyval_raw = abs_cols([v[:, :, q_cols:qkv_cols] for v in qkv_rel])

    def turn_rows(v):
        return rotate(v, positions)

    query_rot, query_pull = jax.vjp(
        turn_rows, query_raw.reshape(rows, HEADS, HD).transpose(1, 0, 2)
    )
    key_rot, key_pull = jax.vjp(turn_rows, keyval_raw[:, :HD])
    queries = query_rot.astype(BF).reshape(HEADS * rows, HD)
    keyval_own = jnp.concatenate([key_rot, keyval_raw[:, HD:]], axis=1).astype(BF)

    column = [keyval_own]
    for _ in range(pairs_back):
        column.append(hop(column[-1], 1))
    beside = [swap(c, "y") for c in column]

    def even_odd(j):
        return (
            jnp.where(odd_y, beside[j], column[j]),
            jnp.where(odd_y, column[j], beside[j]),
        )

    last_even, last_odd = even_odd(pairs_back)
    pieces = [keyval_own, jnp.where(odd_y, beside[0], last_even)]
    places = [seq_place, jnp.where(odd_y, seq_place - 1, 2 * (az - pairs_back))]
    for j in range(1, pairs_back):
        even, odd = even_odd(j)
        pieces += [odd, even]
        places += [2 * (az - j) + 1, 2 * (az - j)]
    pieces.append(last_odd)
    places.append(2 * (az - pairs_back) + 1)
    keyval_all = jnp.concatenate(pieces, axis=0)
    key_rows = keyval_all[:, :HD]
    value_rows = keyval_all[:, HD:]
    key_pos = (jnp.stack(places)[:, None] * rows + token[None, :]).reshape(-1)
    query_pos = jnp.tile(positions, HEADS)
    distance = query_pos[:, None] - key_pos[None, :]
    allowed = (distance >= 0) & (distance < WINDOW) & (key_pos[None, :] >= 0)

    def score_block():
        return jnp.where(allowed, last_last(queries, key_rows) * score_scale, -1e30)

    scores = score_block()
    row_max = jnp.max(scores, axis=1, keepdims=True)
    exponent = jnp.exp(scores - row_max)
    row_total = jnp.sum(exponent, axis=1, keepdims=True)
    probs = exponent / row_total
    log_total = row_max + jnp.log(row_total)
    mixed_heads = jnp.dot(probs.astype(BF), value_rows, preferred_element_type=F32)
    mixed_low = (
        mixed_heads.reshape(HEADS, rows, HD)
        .transpose(1, 0, 2)
        .reshape(rows, HEADS * HD)
        .astype(BF)
    )
    mixed_rel = [v.reshape(rows, z_size * q_cols) for v in rel_cols(mixed_low)]
    resid = inputs + abs_width(times_t(mixed_rel, out_w))
    normed_two_f, norm_two_pull = jax.vjp(norm_rows, resid, gain_two)
    normed_two = normed_two_f.astype(BF)

    cot_got = gather_plane(after(cotangent, keyval_own))
    norm_got = gather_plane(normed_two)
    order = ((0, 0), (1, 0), (0, 1), (1, 1))
    kept = {}
    for k in order:
        cot_g = jnp.concatenate([cot_got[*k, c] for c in (0, 1)], axis=0)
        norm_g = jnp.concatenate([norm_got[*k, c] for c in (0, 1)], axis=0)
        grad_hidden = last_last(cot_g, down_t)
        gate_pre = last_last(norm_g, gate_t)
        upward = last_last(norm_g, up_t)
        gelu_value, gelu_pull = jax.vjp(gelu_tanh, gate_pre)
        hidden = (gelu_value * upward).astype(BF)
        grad_gate = gelu_pull(grad_hidden * upward)[0].astype(BF)
        grad_upward = (grad_hidden * gelu_value).astype(BF)
        kept[k] = (cot_g, norm_g, hidden, grad_gate, grad_upward)

    back = {}
    for k in order[::-1]:
        _, _, _, grad_gate, grad_upward = kept[k]
        part = dot(grad_gate, gate_t, ((1,), (0,))) + dot(grad_upward, up_t, ((1,), (0,)))
        part = part.astype(BF)
        back[k] = (part[:rows], part[rows:])
    grad_normed_two = scatter_plane(back)
    hidden_late, _ = lax.optimization_barrier(
        ({k: kept[k][2] for k in order}, grad_normed_two)
    )
    ahead = {}
    for k in order[::-1]:
        part = dot(hidden_late[k], down_t, ((1,), (0,))).astype(BF)
        ahead[k] = (part[:rows], part[rows:])
    output_rows = (resid + scatter_plane(ahead)).astype(BF)

    kept = after(kept, back)
    cot_all, norm_all, hidden_all, gate_all, upward_all = (
        jnp.concatenate([kept[k][i] for k in order], axis=0) for i in range(5)
    )

    def ff_grad(left, right):
        share = rows_rows(left, right).astype(BF)
        piece = lax.psum_scatter(share, "z", scatter_dimension=0, tiled=True)
        t = piece.reshape(n_hidden, 4, dq).transpose(1, 0, 2)
        t = lax.all_to_all(t, ("x", "c"), split_axis=0, concat_axis=0, tiled=True)
        return t.reshape(ff_cols, dq).T.astype(F32)

    grad_w_gate = ff_grad(gate_all, norm_all)
    grad_w_up = ff_grad(upward_all, norm_all)
    grad_w_down = ff_grad(hidden_all, cot_all)

    grad_resid_part, grad_gain_two = norm_two_pull(grad_normed_two)
    grad_resid = cotangent.astype(F32) + grad_resid_part
    attn_low = rel_blocks(grad_resid.astype(BF))

    def attn_grad(cols, blocks):
        parts = {
            (dx, dy): tuple(rows_rows(cols[dy], blocks[dx, dc]).astype(BF) for dc in (0, 1))
            for dx in (0, 1)
            for dy in (0, 1)
        }
        summed = scatter_plane(parts).astype(BF)
        return lax.psum_scatter(summed, "z", scatter_dimension=0, tiled=True).astype(F32)

    grad_w_out = attn_grad(mixed_rel, attn_low).T
    grad_mixed = abs_cols(
        [v.astype(BF).reshape(rows, z_size, q_cols) for v in times(attn_low, out_w)]
    )
    grad_heads = grad_mixed.reshape(rows, HEADS, HD).transpose(1, 0, 2).reshape(HEADS * rows, HD)
    probs_again = jnp.exp(score_block() - log_total)
    grad_probs = last_last(grad_heads, value_rows)
    grad_scores = (
        probs_again * (grad_probs - jnp.sum(probs_again * grad_probs, axis=1, keepdims=True))
    ).astype(BF)
    grad_keys_all = rows_rows(grad_scores, queries) * score_scale
    grad_values_all = rows_rows(probs_again.astype(BF), grad_heads)
    grad_queries = jnp.dot(grad_scores, key_rows, preferred_element_type=F32) * score_scale
    grad_pieces = jnp.concatenate([grad_keys_all, grad_values_all], axis=1).reshape(
        -1, rows, 2 * HD
    )

    second = grad_pieces[1]
    zero = jnp.zeros_like(second)
    for_column = [grad_pieces[0]]
    for_beside = [jnp.where(odd_y, second, zero)]
    for j in range(1, pairs_back):
        odd, even = grad_pieces[2 * j], grad_pieces[2 * j + 1]
        for_column.append(jnp.where(odd_y, odd, even))
        for_beside.append(jnp.where(odd_y, even, odd))
    last = grad_pieces[-1]
    for_column.append(jnp.where(odd_y, last, second))
    for_beside.append(jnp.where(odd_y, zero, last))
    returned = zero
    for j in range(pairs_back, -1, -1):
        here = for_column[j] + swap(for_beside[j].astype(BF), "y").astype(F32)
        if j < pairs_back:
            here = here + hop(returned.astype(BF), -1).astype(F32)
        returned = here
    grad_keyval = returned
    grad_keys_raw = key_pull(grad_keyval[:, :HD])[0]
    grad_keyval_raw = jnp.concatenate([grad_keys_raw, grad_keyval[:, HD:]], axis=1).astype(BF)
    grad_query_raw = (
        query_pull(grad_queries.reshape(HEADS, rows, HD))[0]
        .transpose(1, 0, 2)
        .reshape(rows, HEADS * HD)
        .astype(BF)
    )
    spare = jnp.zeros((rows, z_size, extra), BF)
    grad_cols = [
        jnp.concatenate([q, kv, spare], axis=2).reshape(rows, z_size * row_size)
        for q, kv in zip(rel_cols(grad_query_raw), rel_cols(grad_keyval_raw))
    ]
    grad_qkv = attn_grad(grad_cols, normed_one)
    grad_w_query = grad_qkv[:q_cols].T
    grad_w_keyval = grad_qkv[q_cols:qkv_cols].T
    grad_normed_one = abs_width(times_t(grad_cols, qkv_w))
    grad_in_part, grad_gain_one = norm_one_pull(grad_normed_one)
    grad_input = grad_resid + grad_in_part
    both = jnp.stack([grad_gain_one, grad_gain_two])
    for axis in ("c", "x", "y"):
        both = both + swap(both, axis)
    both = jnp.sum(lax.all_gather(both, "z"), axis=0)
    place = ((2 * ax + ac) * z_size + az) * 2 + ay
    gain_shares = lax.dynamic_slice_in_dim(both, place * n_gain, n_gain, 1)

    return (
        output_rows,
        grad_input,
        grad_w_query,
        grad_w_keyval,
        grad_w_out,
        gain_shares[0],
        grad_w_gate,
        grad_w_up,
        grad_w_down,
        gain_shares[1],
    )


def solution(mesh):
    n_dp, n_seq = mesh.shape["dp"], mesh.shape["seq"]
    fine = Mesh(mesh.devices.reshape(n_dp // 2, 2, n_seq // 2, 2), ALL)
    tokens = P(ALL, None)
    weight = P(("x", "c"), ("z", "y"))
    gain = P(ALL)
    return jax.shard_map(
        local,
        mesh=fine,
        in_specs=(
            tokens, weight, weight, weight, gain, weight, weight, weight, gain, tokens,
        ),
        out_specs=(
            tokens, tokens, weight, weight, weight, gain, weight, weight, weight, gain,
        ),
        check_vma=False,
    )
```
